32 devices in a mesh: node: 8 (over z, y), local: 4 (over x, core).
Axes of the slice: x: 2, y: 2, z: 4, core: 2. Of those that a mesh axis runs over, the one named last changes fastest.
Arguments:
- tokens: bfloat16 [4096, 7168], P(('node', 'local')), may hold values from -6 to 6
- w_gate: bfloat16 [8, 7168, 1024], P('node', None, 'local'), may hold values from -0.0625 to 0.0625
- w_up: bfloat16 [8, 7168, 1024], P('node', None, 'local'), may hold values from -0.0625 to 0.0625
- w_down: bfloat16 [8, 1024, 7168], P('node', 'local'), may hold values from -0.1875 to 0.1875
- chosen: int32 [8, 48], replicated, may hold values from 0 to 4095, as said below
- counts: int32 [8], replicated, may hold values from 3 to 48, as said below
- gates: float32 [8, 48], replicated, may hold values from 0.2 to 1
Outputs:
- mixed: bfloat16 [4096, 7168], P(('node', 'local'))
The draws below stay inside these ranges and needn't reach their ends.
Inputs may be any that keep to these rules, and one draw needn't show every extreme that they name: `chosen`: each expert's list holds distinct tokens; in each list at most 3 entries lie in one device's block of 128 consecutive tokens, and for every expert some block holds exactly 3 live entries. `counts`: some expert has exactly 48 live entries.
All inputs are finite; a program needn't handle non-finite values.
Results may differ from the reference program's by a relative error of at most 0.014.
Values may be sent and summed in bfloat16 or wider, within the bound.
A program may use at most 128 MiB of HBM per device.

```python
import jax
import jax.numpy as jnp
from jax import lax

D = 7168
FF = 1024
SLOT = 3
TOK_DEV = 128
EXPERTS = 8
TOKENS = 4096
CAP = 48
FF_DEV = 256
N_LOCAL = 4


def lists_for(key):
    base = jax.random.fold_in(key, 11)
    many = TOKENS // TOK_DEV

    def one_list(index):
        sub = jax.random.fold_in(base, index)
        first, second, third, fourth = jax.random.split(sub, 4)
        heavy = jax.random.randint(first, (), 0, many)
        places = jnp.arange(many * SLOT, dtype=jnp.int32)
        owner = places // SLOT
        ranks = jax.random.permutation(second, many * SLOT).astype(jnp.int32)
        score = ranks - jnp.where(owner == heavy, many * SLOT, 0)
        order = jnp.argsort(score, stable=True)[:CAP]
        within = jax.random.permutation(third, TOK_DEV)[:SLOT].astype(jnp.int32)
        offsets = jax.random.randint(fourth, (many,), 0, TOK_DEV)
        position = (within[places % SLOT] + offsets[owner]) % TOK_DEV
        token = owner * TOK_DEV + position
        return token[order].astype(jnp.int32)
    return jax.vmap(one_list)(jnp.arange(EXPERTS, dtype=jnp.int32))


def draw_chosen(key, part):
    return lists_for(key)


def draw_counts(key, part):
    sub = jax.random.fold_in(key, 23)
    first, second = jax.random.split(sub)
    values = jax.random.randint(first, (EXPERTS,), 3 * CAP // 4, CAP + 1)
    full = jax.random.randint(second, (), 0, EXPERTS)
    return jnp.where(jnp.arange(EXPERTS) == full, CAP, values).astype(jnp.int32)


def shard_levels(own_key, shape, cuts, least, largest):
    gain, own = 1.0, jax.random.fold_in(own_key, 6)
    for axis_at, blocks in cuts:
        steps = jnp.exp(jax.random.uniform(jax.random.fold_in(own, axis_at), (blocks,), jnp.float32, least / len(cuts), largest / len(cuts)))
        gain = gain * jnp.repeat(steps, shape[axis_at] // blocks).reshape([-1 if axis == axis_at else 1 for axis in range(len(shape))])
    return gain


def gaussian(own_key, extent, width, limit, cuts=(), held_as=jnp.bfloat16):
    entries = jax.random.normal(own_key, extent, jnp.float32) * width
    if len(cuts) > 0:
        entries = shard_levels(own_key, extent, cuts, -0.22, 0.18) * entries
    return jnp.clip(entries, min=-limit, max=limit).astype(held_as)


def setup_inputs(seed: int = 0) -> dict:
    keys = jax.random.split(jax.random.key(seed), 8)
    return {
        "tokens": gaussian(keys[0], (TOKENS, D), 1.0, 6.0, ((0, 32),)),
        "w_gate": gaussian(keys[1], (EXPERTS, D, FF), D ** -0.5, 0.0625, ((0, 8), (2, 4))),
        "w_up": gaussian(keys[2], (EXPERTS, D, FF), D ** -0.5, 0.0625, ((0, 8), (2, 4))),
        "w_down": gaussian(keys[3], (EXPERTS, FF, D), FF ** -0.5, 0.1875, ((0, 8), (1, 4))),
        "chosen": draw_chosen(jax.random.fold_in(keys[7], 71), 0),
        "counts": draw_counts(jax.random.fold_in(keys[7], 71), 0),
        "gates": jnp.clip(jax.random.uniform(keys[6], (EXPERTS, CAP), jnp.float32, 0.2, 1.0), 0.2, 1.0),
    }


def reference(tokens, w_gate, w_up, w_down, chosen, counts, gates):
    def one_expert(total, item):
        gate_mat, up_mat, down_mat, picked, count, weight = item
        rows = tokens[picked]
        live = jnp.arange(CAP, dtype=jnp.int32) < count
        scale = jnp.where(live, weight, jnp.float32(0.0))
        answer = jnp.zeros((CAP, D), jnp.float32)
        for group in range(N_LOCAL):
            low = group * FF_DEV
            gate_val = jnp.dot(rows, gate_mat[:, low:low + FF_DEV], preferred_element_type=jnp.float32)
            up_val = jnp.dot(rows, up_mat[:, low:low + FF_DEV], preferred_element_type=jnp.float32)
            hidden = (jax.nn.silu(gate_val) * up_val).astype(jnp.bfloat16)
            down_val = jnp.dot(hidden, down_mat[low:low + FF_DEV, :], preferred_element_type=jnp.float32)
            part = (scale[:, None] * down_val).astype(jnp.bfloat16)
            answer = answer + part.astype(jnp.float32)
        answer = answer.astype(jnp.bfloat16).astype(jnp.float32)
        answer = jnp.where(live[:, None], answer, jnp.float32(0.0))
        return total.at[picked].add(answer), None

    start = jnp.zeros((TOKENS, D), jnp.float32)
    total, _ = lax.scan(one_expert, start, (w_gate, w_up, w_down, chosen, counts, gates))
    return total.astype(jnp.bfloat16)
```

```python
import functools

import jax
import jax.numpy as jnp
from jax import lax
from jax.experimental import pallas as pl
from jax.experimental.pallas import tpu as pltpu
from jax.sharding import PartitionSpec as P

SLOT = 3
SUB, LANE = 8, 128
COLS = SUB * LANE
MESH = pl.DeviceIdType.MESH
DISPATCH_GROUPS = 2
COMBINE_GROUPS = 4


def split(count, groups):
    groups = min(groups, count)
    sizes = [count // groups + (1 if g < count % groups else 0) for g in range(groups)]
    starts = [sum(sizes[:g]) for g in range(groups)]
    return list(zip(starts, sizes))


def kernel(dims, counts_ref, chosen_ref, gates_ref, tokens_ref, wg_hbm, wu_hbm, wd_hbm, out_ref,
           wg, wu, wd, tx, rx, py, r1b, s2, r2b, a3, ax, stage,
           wsem, lsem, bsem, d1s, d1r, d2s, d2r, d3s, d3r, d4s, d4r, r1s, r1r, r2s, r2r, r3s, r3r):
    n_node, n_local, chunks, tok_dev, ff = dims
    nx = n_local // 2
    experts, cap = chosen_ref.shape
    per = n_node * SLOT
    rows = n_local * per
    f32, bf16 = jnp.float32, jnp.bfloat16
    me_n, me_l = lax.axis_index("node"), lax.axis_index("local")
    me_x, me_c = me_l // 2, me_l % 2
    partner = me_x * 2 + (1 - me_c)
    dgroups, cgroups = split(chunks, DISPATCH_GROUPS), split(chunks, COMBINE_GROUPS)

    def node_at(k):
        return lax.rem(me_n + k + n_node, n_node)

    def x_at(k):
        return lax.rem(me_x + k + nx, nx)

    def remote(src, dst, ssem, rsem, node, local):
        return pltpu.make_async_remote_copy(
            src_ref=src, dst_ref=dst, send_sem=ssem, recv_sem=rsem,
            device_id=(node, local), device_id_type=MESH)

    sent = []

    def send(*args):
        copy = remote(*args)
        copy.start()
        sent.append(copy)

    barrier = pltpu.get_barrier_semaphore()
    for k in range(1, n_node):
        pl.semaphore_signal(barrier, inc=1, device_id=(node_at(k), me_l), device_id_type=MESH)
    pl.semaphore_signal(barrier, inc=1, device_id=(me_n, partner), device_id_type=MESH)
    for k in range(1, nx):
        pl.semaphore_signal(barrier, inc=1, device_id=(me_n, x_at(k) * 2 + me_c), device_id_type=MESH)

    loads = [pltpu.make_async_copy(src.at[0], dst, wsem.at[i])
             for i, (src, dst) in enumerate(((wg_hbm, wg), (wu_hbm, wu), (wd_hbm, wd)))]
    for copy in loads:
        copy.start()

    base = (me_n * n_local + me_l) * tok_dev
    row = lax.broadcasted_iota(jnp.int32, (experts, cap), 0)
    count = jnp.zeros((experts, cap), jnp.int32)
    for e in range(experts):
        count = jnp.where(row == e, counts_ref[e], count)
    pos = chosen_ref[...] - base
    mine = (lax.broadcasted_iota(jnp.int32, (experts, cap), 1) < count) & (pos >= 0) & (pos < tok_dev)
    before = (lax.broadcasted_iota(jnp.int32, (cap, cap), 0)
              < lax.broadcasted_iota(jnp.int32, (cap, cap), 1))
    rank = jnp.dot(jnp.where(mine, 1.0, 0.0).astype(bf16), jnp.where(before, 1.0, 0.0).astype(bf16),
                   preferred_element_type=f32)
    pos1 = (pos + 1).astype(f32)
    lane1 = (lax.broadcasted_iota(jnp.int32, (experts, tok_dev), 1) + 1).astype(f32)
    picks, weights = [], []
    for s in range(SLOT):
        sel = mine & (rank == float(s))
        where = jnp.sum(jnp.where(sel, pos1, 0.0), axis=1, keepdims=True)
        gate = jnp.sum(jnp.where(sel, gates_ref[...], 0.0), axis=1, keepdims=True)
        hit = lane1 == where
        picks.append(jnp.where(hit, 1.0, 0.0))
        weights.append(jnp.where(hit, gate, 0.0))
    pick = jnp.concatenate(picks, axis=0)
    weight = jnp.concatenate(weights, axis=0)
    col = lax.broadcasted_iota(jnp.int32, (per, per), 1)
    slot = jnp.zeros((per, per), jnp.int32)
    for s in range(1, SLOT):
        slot = slot + jnp.where(col >= s * experts, 1, 0)
    order = lax.broadcasted_iota(jnp.int32, (per, per), 0) == (col - slot * experts) * SLOT + slot
    order = jnp.where(order, 1.0, 0.0).astype(bf16)
    high = weight.astype(bf16)
    low = (weight - high.astype(f32)).astype(bf16)

    def ordered(x):
        return jnp.dot(order, x, preferred_element_type=f32)

    select = ordered(pick.astype(bf16)).astype(bf16)
    high_t = jnp.transpose(ordered(high)).astype(bf16)
    low_t = jnp.transpose(ordered(low)).astype(bf16)

    def to_tiles(value, m):
        for q in range(SUB):
            stage[pl.ds(q, m, stride=SUB), :] = value[:, q * LANE:(q + 1) * LANE]
        return stage[pl.ds(0, m * SUB), :].astype(bf16).reshape(m, SUB, LANE)

    def from_tiles(value, m):
        stage[pl.ds(0, m * SUB), :] = value.reshape(m * SUB, LANE).astype(f32)
        return jnp.concatenate(
            [stage[pl.ds(q, m, stride=SUB), :].astype(bf16) for q in range(SUB)], axis=1)

    mine_rows = pl.ds(me_n * SLOT, SLOT)
    far_first = list(range(1, n_node))
    far_first.sort(key=lambda k: -min(k, n_node - k))
    own = []
    for g, (j0, jn) in enumerate(dgroups):
        js = pl.ds(j0, jn)
        for j in range(j0, j0 + jn):
            picked = jnp.dot(select, tokens_ref[:, j * COLS:(j + 1) * COLS], preferred_element_type=f32)
            tx[j] = to_tiles(picked, per)
        if g == 0:
            pl.semaphore_wait(barrier, n_node - 1 + 1 + nx - 1)
        for k in far_first:
            dst = node_at(k)
            send(tx.at[js, pl.ds(dst * SLOT, SLOT)], rx.at[js, me_l, mine_rows],
                 d1s.at[g, k], d1r.at[g, k], dst, me_l)
        copy = pltpu.make_async_copy(tx.at[js, mine_rows], rx.at[js, me_l, mine_rows], lsem.at[g])
        copy.start()
        own.append(copy)

    near_first = [0] + far_first[::-1]

    def block(js, local, node):
        return rx.at[js, local, pl.ds(node * SLOT, SLOT)]

    def pass_on(g):
        j0, jn = dgroups[g]
        js = pl.ds(j0, jn)
        for k in near_first:
            src = node_at(-k)
            here = block(js, me_l, src)
            if k == 0:
                out = tx.at[js, mine_rows]
            else:
                remote(here, here, d1s.at[g, k], d1r.at[g, k], me_n, partner).wait_recv()
                out = here
            for d in range(1, nx):
                send(out, here, d2s.at[g, k, d], d2r.at[g, k, d], me_n, x_at(d) * 2 + me_c)
            send(out, here, d3s.at[g, k], d3r.at[g, k], me_n, partner)

    def pass_across(g):
        j0, jn = dgroups[g]
        js = pl.ds(j0, jn)
        for k in near_first:
            src = node_at(-k)
            for d in range(1, nx):
                here = block(js, x_at(-d) * 2 + me_c, src)
                remote(here, here, d2s.at[g, k, d], d2r.at[g, k, d], me_n, partner).wait_recv()
                send(here, here, d4s.at[g, k, d], d4r.at[g, k, d], me_n, partner)

    def wait_rest(g):
        j0, jn = dgroups[g]
        js = pl.ds(j0, jn)
        own[g].wait()
        for k in near_first:
            src = node_at(-k)
            here = block(js, partner, src)
            remote(here, here, d3s.at[g, k], d3r.at[g, k], me_n, partner).wait_recv()
            for d in range(1, nx):
                here = block(js, x_at(-d) * 2 + (1 - me_c), src)
                remote(here, here, d4s.at[g, k, d], d4r.at[g, k, d], me_n, partner).wait_recv()

    acc = (jnp.zeros((rows, ff), f32), jnp.zeros((rows, ff), f32))

    def first_matmuls(g, acc):
        j0, jn = dgroups[g]

        def step(j, acc):
            x = from_tiles(rx[j].reshape(rows, SUB, LANE), rows)
            ks = pl.ds(pl.multiple_of(j * COLS, COLS), COLS)
            return (acc[0] + jnp.dot(x, wg[ks, :], preferred_element_type=f32),
                    acc[1] + jnp.dot(x, wu[ks, :], preferred_element_type=f32))
        return lax.fori_loop(j0, j0 + jn, step, acc)

    for g in range(len(dgroups)):
        pass_on(g)
        if g > 0:
            pass_across(g - 1)
    pass_across_last = len(dgroups) - 1
    for g in range(len(dgroups)):
        if g == pass_across_last:
            pass_across(g)
        wait_rest(g)
        if g == 0:
            loads[0].wait()
            loads[1].wait()
        acc = first_matmuls(g, acc)
    hidden = (acc[0] / (1.0 + jnp.exp(-acc[0])) * acc[1]).astype(bf16)
    loads[2].wait()

    octs = per // SUB
    for g, (j0, jn) in enumerate(cgroups):
        js = pl.ds(j0, jn)
        for j in range(j0, j0 + jn):
            y = jnp.dot(hidden, wd[:, j * COLS:(j + 1) * COLS], preferred_element_type=f32)
            py[j] = y.reshape(n_local, octs, SUB, COLS).astype(bf16)
        for xx in range(nx):
            send(py.at[js, xx * 2 + (1 - me_c)], r1b.at[js, xx], r1s.at[g, xx], r1r.at[g, xx], me_n, partner)
    for g, (j0, jn) in enumerate(cgroups):
        js = pl.ds(j0, jn)
        for xx in range(nx):
            there = r1b.at[js, xx]
            remote(there, there, r1s.at[g, xx], r1r.at[g, xx], me_n, partner).wait_recv()
        for d in range(1, nx):
            xd = x_at(d)
            for j in range(j0, j0 + jn):
                s2[j, d - 1] = (py[j, xd * 2 + me_c].astype(f32) + r1b[j, xd].astype(f32)).astype(bf16)
            send(s2.at[js, d - 1], r2b.at[js, d - 1], r2s.at[g, d], r2r.at[g, d], me_n, xd * 2 + me_c)
    back = []
    for g, (j0, jn) in enumerate(cgroups):
        js = pl.ds(j0, jn)
        for d in range(1, nx):
            there = r2b.at[js, d - 1]
            remote(there, there, r2s.at[g, d], r2r.at[g, d], me_n, partner).wait_recv()
        for j in range(j0, j0 + jn):
            total = py[j, me_l].astype(f32) + r1b[j, me_x].astype(f32)
            for d in range(1, nx):
                total = total + r2b[j, d - 1].astype(f32)
            a3[j] = to_tiles(total.reshape(per, COLS), per)
        for k in far_first:
            dst = node_at(k)
            send(a3.at[js, pl.ds(dst * SLOT, SLOT)], ax.at[js, mine_rows],
                 r3s.at[g, k], r3r.at[g, k], dst, me_l)
        copy = pltpu.make_async_copy(a3.at[js, mine_rows], ax.at[js, mine_rows], bsem.at[g])
        copy.start()
        back.append(copy)
    for g, (j0, jn) in enumerate(cgroups):
        js = pl.ds(j0, jn)
        back[g].wait()
        for k in near_first[1:]:
            there = ax.at[js, pl.ds(node_at(-k) * SLOT, SLOT)]
            remote(there, there, r3s.at[g, k], r3r.at[g, k], me_n, partner).wait_recv()
        for j in range(j0, j0 + jn):
            answers = from_tiles(ax[j], per)
            mixed = (jnp.dot(high_t, answers, preferred_element_type=f32)
                     + jnp.dot(low_t, answers, preferred_element_type=f32))
            out_ref[:, j * COLS:(j + 1) * COLS] = mixed.astype(bf16)
    for copy in sent:
        copy.wait_send()


def shards(n_node, n_local, tokens, w_gate, w_up, w_down, chosen, counts, gates):
    tok_dev, width = tokens.shape
    ff = w_gate.shape[2]
    chunks = width // COLS
    nx = n_local // 2
    per = n_node * SLOT
    octs = per // SUB
    rows = n_local * per
    dg, cg = len(split(chunks, DISPATCH_GROUPS)), len(split(chunks, COMBINE_GROUPS))
    bf16 = jnp.bfloat16
    vmem = pl.BlockSpec(memory_space=pltpu.VMEM)
    dma = pltpu.SemaphoreType.DMA
    xs = max(nx - 1, 1)
    return pl.pallas_call(
        functools.partial(kernel, (n_node, n_local, chunks, tok_dev, ff)),
        out_shape=jax.ShapeDtypeStruct((tok_dev, width), bf16),
        in_specs=[pl.BlockSpec(memory_space=pltpu.SMEM), vmem, vmem, vmem]
        + [pl.BlockSpec(memory_space=pl.ANY)] * 3,
        out_specs=vmem,
        scratch_shapes=[
            pltpu.VMEM((width, ff), bf16),
            pltpu.VMEM((width, ff), bf16),
            pltpu.VMEM((ff, width), bf16),
            pltpu.VMEM((chunks, per, SUB, LANE), bf16),
            pltpu.VMEM((chunks, n_local, per, SUB, LANE), bf16),
            pltpu.VMEM((chunks, n_local, octs, SUB, COLS), bf16),
            pltpu.VMEM((chunks, nx, octs, SUB, COLS), bf16),
            pltpu.VMEM((chunks, xs, octs, SUB, COLS), bf16),
            pltpu.VMEM((chunks, xs, octs, SUB, COLS), bf16),
            pltpu.VMEM((chunks, per, SUB, LANE), bf16),
            pltpu.VMEM((chunks, per, SUB, LANE), bf16),
            pltpu.VMEM((rows * SUB, LANE), jnp.float32),
            dma((3,)), dma((dg,)), dma((cg,)),
            dma((dg, n_node)), dma((dg, n_node)),
            dma((dg, n_node, nx)), dma((dg, n_node, nx)),
            dma((dg, n_node)), dma((dg, n_node)),
            dma((dg, n_node, nx)), dma((dg, n_node, nx)),
            dma((cg, nx)), dma((cg, nx)),
            dma((cg, nx)), dma((cg, nx)),
            dma((cg, n_node)), dma((cg, n_node)),
        ],
        compiler_params=pltpu.CompilerParams(
            collective_id=0, has_side_effects=True, vmem_limit_bytes=66000000),
    )(counts, chosen, gates, tokens, w_gate, w_up, w_down)


def solution(mesh):
    in_specs = (
        P(("node", "local"), None),
        P("node", None, "local"),
        P("node", None, "local"),
        P("node", "local", None),
        P(),
        P(),
        P(),
    )
    out_specs = P(("node", "local"), None)
    body = functools.partial(shards, mesh.shape["node"], mesh.shape["local"])
    return jax.shard_map(body, mesh=mesh, in_specs=in_specs, out_specs=out_specs, check_vma=False)
```

```python
import functools

import jax
import jax.numpy as jnp
from jax import lax
from jax.experimental import pallas as pl
from jax.experimental.pallas import tpu as pltpu
from jax.sharding import PartitionSpec as P

SLOT = 3
SUB, LANE = 8, 128
COLS = SUB * LANE
MESH = pl.DeviceIdType.MESH
DISPATCH_GROUPS = 1
COMBINE_GROUPS = 4


def split(count, groups):
    groups = min(groups, count)
    sizes = [count // groups + (1 if g < count % groups else 0) for g in range(groups)]
    starts = [sum(sizes[:g]) for g in range(groups)]
    return list(zip(starts, sizes))


def kernel(dims, counts_hbm, chosen_hbm, gates_hbm, tokens_hbm, wg_hbm, wu_hbm, wd_hbm, out_ref, place_ref,
           counts_ref, chosen_ref, gates_ref, tokens_ref, wg, wu, wd, tx, rx, py, r1b, s2, r2b, a3, ax, stage,
           wsem, lsem, bsem, d1s, d1r, d2s, d2r, d3s, d3r, d4s, d4r, r1s, r1r, r2s, r2r, r3s, r3r):
    n_node, n_local, chunks, tok_dev, ff = dims
    nx = n_local // 2
    experts, cap = chosen_ref.shape
    per = n_node * SLOT
    rows = n_local * per
    padded = out_ref.shape[0] // 2
    f32, bf16 = jnp.float32, jnp.bfloat16
    me_n, me_l = lax.axis_index("node"), lax.axis_index("local")
    me_x, me_c = me_l // 2, me_l % 2
    partner = me_x * 2 + (1 - me_c)
    dgroups, cgroups = split(chunks, DISPATCH_GROUPS), split(chunks, COMBINE_GROUPS)

    paired = n_node & (n_node - 1) == 0

    def node_at(k):
        if paired:
            return jnp.bitwise_xor(me_n, abs(k))
        return lax.rem(me_n + k + n_node, n_node)

    def x_at(k):
        return lax.rem(me_x + k + nx, nx)

    def remote(src, dst, ssem, rsem, node, local):
        return pltpu.make_async_remote_copy(
            src_ref=src, dst_ref=dst, send_sem=ssem, recv_sem=rsem,
            device_id=(node, local), device_id_type=MESH)

    sent = []

    def send(*args):
        copy = remote(*args)
        copy.start()
        sent.append(copy)

    barrier = pltpu.get_barrier_semaphore()
    for k in range(1, n_node):
        pl.semaphore_signal(barrier, inc=1, device_id=(node_at(k), me_l), device_id_type=MESH)
    pl.semaphore_signal(barrier, inc=1, device_id=(me_n, partner), device_id_type=MESH)
    for k in range(1, nx):
        pl.semaphore_signal(barrier, inc=1, device_id=(me_n, x_at(k) * 2 + me_c), device_id_type=MESH)

    loads = [pltpu.make_async_copy(src, dst, wsem.at[i]) for i, (src, dst) in enumerate((
        (wg_hbm.at[0], wg), (wu_hbm.at[0], wu), (wd_hbm.at[0], wd), (tokens_hbm, tokens_ref),
        (counts_hbm, counts_ref), (chosen_hbm, chosen_ref), (gates_hbm, gates_ref)))]
    for copy in loads[4:] + [loads[3]] + loads[:3]:
        copy.start()
    for copy in loads[4:]:
        copy.wait()

    base = (me_n * n_local + me_l) * tok_dev
    row = lax.broadcasted_iota(jnp.int32, (experts, cap), 0)
    count = jnp.zeros((experts, cap), jnp.int32)
    for e in range(experts):
        count = jnp.where(row == e, counts_ref[e], count)
    pos = chosen_ref[...] - base
    mine = (lax.broadcasted_iota(jnp.int32, (experts, cap), 1) < count) & (pos >= 0) & (pos < tok_dev)
    before = (lax.broadcasted_iota(jnp.int32, (cap, cap), 0)
              < lax.broadcasted_iota(jnp.int32, (cap, cap), 1))
    rank = jnp.dot(jnp.where(mine, 1.0, 0.0).astype(bf16), jnp.where(before, 1.0, 0.0).astype(bf16),
                   preferred_element_type=f32)
    pos1 = (pos + 1).astype(f32)
    lane1 = (lax.broadcasted_iota(jnp.int32, (experts, tok_dev), 1) + 1).astype(f32)
    picks, weights = [], []
    for s in range(SLOT):
        sel = mine & (rank == float(s))
        where = jnp.sum(jnp.where(sel, pos1, 0.0), axis=1, keepdims=True)
        gate = jnp.sum(jnp.where(sel, gates_ref[...], 0.0), axis=1, keepdims=True)
        hit = lane1 == where
        picks.append(jnp.where(hit, 1.0, 0.0))
        weights.append(jnp.where(hit, gate, 0.0))
    pick = jnp.concatenate(picks, axis=0)
    weight = jnp.concatenate(weights, axis=0)
    col = lax.broadcasted_iota(jnp.int32, (per, per), 1)
    slot = jnp.zeros((per, per), jnp.int32)
    for s in range(1, SLOT):
        slot = slot + jnp.where(col >= s * experts, 1, 0)
    order = lax.broadcasted_iota(jnp.int32, (per, per), 0) == (col - slot * experts) * SLOT + slot
    order = jnp.where(order, 1.0, 0.0).astype(bf16)
    high = weight.astype(bf16)
    low = (weight - high.astype(f32)).astype(bf16)

    def ordered(x):
        return jnp.dot(order, x, preferred_element_type=f32)

    select = ordered(pick.astype(bf16)).astype(bf16)
    fill = jnp.zeros((padded - per, tok_dev), f32)
    parts = [ordered(high), fill, ordered(low), fill] if padded > per else [ordered(high), ordered(low)]
    place_ref[...] = jnp.transpose(jnp.concatenate(parts, axis=0)).astype(bf16)
    if padded > per:
        out_ref[...] = jnp.zeros_like(out_ref)

    def to_tiles(value, m):
        for q in range(SUB):
            stage[pl.ds(q, m, stride=SUB), :] = value[:, q * LANE:(q + 1) * LANE]
        return stage[pl.ds(0, m * SUB), :].astype(bf16).reshape(m, SUB, LANE)

    def from_tiles(value, m):
        stage[pl.ds(0, m * SUB), :] = value.reshape(m * SUB, LANE).astype(f32)
        return jnp.concatenate(
            [stage[pl.ds(q, m, stride=SUB), :].astype(bf16) for q in range(SUB)], axis=1)

    mine_rows = pl.ds(me_n * SLOT, SLOT)
    near_first = list(range(n_node))
    far_first = near_first[:0:-1]
    own = []
    loads[3].wait()
    for g, (j0, jn) in enumerate(dgroups):
        js = pl.ds(j0, jn)
        for j in range(j0, j0 + jn):
            picked = jnp.dot(select, tokens_ref[:, j * COLS:(j + 1) * COLS], preferred_element_type=f32)
            tx[j] = to_tiles(picked, per)
        if g == 0:
            pl.semaphore_wait(barrier, n_node - 1 + 1 + nx - 1)
        for k in near_first[1:]:
            dst = node_at(k)
            send(tx.at[js, pl.ds(dst * SLOT, SLOT)], rx.at[js, me_l, mine_rows],
                 d1s.at[g, k], d1r.at[g, k], dst, me_l)
        copy = pltpu.make_async_copy(tx.at[js, mine_rows], rx.at[js, me_l, mine_rows], lsem.at[g])
        copy.start()
        own.append(copy)


    def block(js, local, node):
        return rx.at[js, local, pl.ds(node * SLOT, SLOT)]

    def pass_on(g):
        j0, jn = dgroups[g]
        js = pl.ds(j0, jn)
        for k in near_first:
            src = node_at(-k)
            here = block(js, me_l, src)
            if k == 0:
                out = tx.at[js, mine_rows]
            else:
                remote(here, here, d1s.at[g, k], d1r.at[g, k], me_n, partner).wait_recv()
                out = here
            for d in range(1, nx):
                send(out, here, d2s.at[g, k, d], d2r.at[g, k, d], me_n, x_at(d) * 2 + me_c)
            send(out, here, d3s.at[g, k], d3r.at[g, k], me_n, partner)

    def pass_across(g):
        j0, jn = dgroups[g]
        js = pl.ds(j0, jn)
        for k in near_first:
            src = node_at(-k)
            for d in range(1, nx):
                here = block(js, x_at(-d) * 2 + me_c, src)
                remote(here, here, d2s.at[g, k, d], d2r.at[g, k, d], me_n, partner).wait_recv()
                send(here, here, d4s.at[g, k, d], d4r.at[g, k, d], me_n, partner)

    def wait_rest(g):
        j0, jn = dgroups[g]
        js = pl.ds(j0, jn)
        own[g].wait()
        for k in near_first:
            src = node_at(-k)
            here = block(js, partner, src)
            remote(here, here, d3s.at[g, k], d3r.at[g, k], me_n, partner).wait_recv()
            for d in range(1, nx):
                here = block(js, x_at(-d) * 2 + (1 - me_c), src)
                remote(here, here, d4s.at[g, k, d], d4r.at[g, k, d], me_n, partner).wait_recv()

    acc = (jnp.zeros((rows, ff), f32), jnp.zeros((rows, ff), f32))

    def first_matmuls(g, acc):
        j0, jn = dgroups[g]

        def step(j, acc):
            x = from_tiles(rx[j].reshape(rows, SUB, LANE), rows)
            ks = pl.ds(pl.multiple_of(j * COLS, COLS), COLS)
            return (acc[0] + jnp.dot(x, wg[ks, :], preferred_element_type=f32),
                    acc[1] + jnp.dot(x, wu[ks, :], preferred_element_type=f32))
        return lax.fori_loop(j0, j0 + jn, step, acc)

    for g in range(len(dgroups)):
        pass_on(g)
        if g > 0:
            pass_across(g - 1)
    pass_across_last = len(dgroups) - 1
    for g in range(len(dgroups)):
        if g == pass_across_last:
            pass_across(g)
        wait_rest(g)
        if g == 0:
            loads[0].wait()
            loads[1].wait()
        acc = first_matmuls(g, acc)
    hidden = (acc[0] / (1.0 + jnp.exp(-acc[0])) * acc[1]).astype(bf16)
    loads[2].wait()

    octs = per // SUB
    for g, (j0, jn) in enumerate(cgroups):
        js = pl.ds(j0, jn)
        for j in range(j0, j0 + jn):
            y = jnp.dot(hidden, wd[:, j * COLS:(j + 1) * COLS], preferred_element_type=f32)
            py[j] = y.reshape(n_local, octs, SUB, COLS).astype(bf16)
        for xx in range(nx):
            send(py.at[js, xx * 2 + (1 - me_c)], r1b.at[js, xx], r1s.at[g, xx], r1r.at[g, xx], me_n, partner)
    for g, (j0, jn) in enumerate(cgroups):
        js = pl.ds(j0, jn)
        for xx in range(nx):
            there = r1b.at[js, xx]
            remote(there, there, r1s.at[g, xx], r1r.at[g, xx], me_n, partner).wait_recv()
        for d in range(1, nx):
            xd = x_at(d)
            for j in range(j0, j0 + jn):
                s2[j, d - 1] = (py[j, xd * 2 + me_c].astype(f32) + r1b[j, xd].astype(f32)).astype(bf16)
            send(s2.at[js, d - 1], r2b.at[js, d - 1], r2s.at[g, d], r2r.at[g, d], me_n, xd * 2 + me_c)
    back = []
    for g, (j0, jn) in enumerate(cgroups):
        js = pl.ds(j0, jn)
        for d in range(1, nx):
            there = r2b.at[js, d - 1]
            remote(there, there, r2s.at[g, d], r2r.at[g, d], me_n, partner).wait_recv()
        for j in range(j0, j0 + jn):
            total = py[j, me_l].astype(f32) + r1b[j, me_x].astype(f32)
            for d in range(1, nx):
                total = total + r2b[j, d - 1].astype(f32)
            a3[j] = to_tiles(total.reshape(per, COLS), per)
        for k in far_first:
            dst = node_at(k)
            send(a3.at[js, pl.ds(dst * SLOT, SLOT)], ax.at[js, mine_rows],
                 r3s.at[g, k], r3r.at[g, k], dst, me_l)
        copy = pltpu.make_async_copy(a3.at[js, mine_rows], ax.at[js, mine_rows], bsem.at[g])
        copy.start()
        back.append(copy)
    for g, (j0, jn) in enumerate(cgroups):
        js = pl.ds(j0, jn)
        back[g].wait()
        for k in near_first[1:]:
            there = ax.at[js, pl.ds(node_at(-k) * SLOT, SLOT)]
            remote(there, there, r3s.at[g, k], r3r.at[g, k], me_n, partner).wait_recv()
        for j in range(j0, j0 + jn):
            answers = from_tiles(ax[j], per)
            out_ref[0:per, j * COLS:(j + 1) * COLS] = answers
            out_ref[padded:padded + per, j * COLS:(j + 1) * COLS] = answers
    for copy in sent:
        copy.wait_send()


def mix(place_ref, answers_ref, out_ref):
    answers = answers_ref[...]
    mixed = (jnp.dot(place_ref[0], answers, preferred_element_type=jnp.float32)
             + jnp.dot(place_ref[1], answers, preferred_element_type=jnp.float32))
    out_ref[...] = mixed.astype(out_ref.dtype)


def shards(n_node, n_local, tokens, w_gate, w_up, w_down, chosen, counts, gates):
    tok_dev, width = tokens.shape
    ff = w_gate.shape[2]
    chunks = width // COLS
    nx = n_local // 2
    per = n_node * SLOT
    octs = per // SUB
    padded = -(-per // 16) * 16
    rows = n_local * per
    dg, cg = len(split(chunks, DISPATCH_GROUPS)), len(split(chunks, COMBINE_GROUPS))
    bf16 = jnp.bfloat16
    vmem = pl.BlockSpec(memory_space=pltpu.VMEM)
    dma = pltpu.SemaphoreType.DMA
    xs = max(nx - 1, 1)
    answers, place = pl.pallas_call(
        functools.partial(kernel, (n_node, n_local, chunks, tok_dev, ff)),
        out_shape=(jax.ShapeDtypeStruct((2 * padded, width), bf16), jax.ShapeDtypeStruct((tok_dev, 2 * padded), bf16)),
        in_specs=[pl.BlockSpec(memory_space=pl.ANY)] * 7,
        out_specs=(vmem, vmem),
        scratch_shapes=[
            pltpu.SMEM(counts.shape, counts.dtype),
            pltpu.VMEM(chosen.shape, chosen.dtype),
            pltpu.VMEM(gates.shape, gates.dtype),
            pltpu.VMEM((tok_dev, width), bf16),
            pltpu.VMEM((width, ff), bf16),
            pltpu.VMEM((width, ff), bf16),
            pltpu.VMEM((ff, width), bf16),
            pltpu.VMEM((chunks, per, SUB, LANE), bf16),
            pltpu.VMEM((chunks, n_local, per, SUB, LANE), bf16),
            pltpu.VMEM((chunks, n_local, octs, SUB, COLS), bf16),
            pltpu.VMEM((chunks, nx, octs, SUB, COLS), bf16),
            pltpu.VMEM((chunks, xs, octs, SUB, COLS), bf16),
            pltpu.VMEM((chunks, xs, octs, SUB, COLS), bf16),
            pltpu.VMEM((chunks, per, SUB, LANE), bf16),
            pltpu.VMEM((chunks, per, SUB, LANE), bf16),
            pltpu.VMEM((rows * SUB, LANE), jnp.float32),
            dma((7,)), dma((dg,)), dma((cg,)),
            dma((dg, n_node)), dma((dg, n_node)),
            dma((dg, n_node, nx)), dma((dg, n_node, nx)),
            dma((dg, n_node)), dma((dg, n_node)),
            dma((dg, n_node, nx)), dma((dg, n_node, nx)),
            dma((cg, nx)), dma((cg, nx)),
            dma((cg, nx)), dma((cg, nx)),
            dma((cg, n_node)), dma((cg, n_node)),
        ],
        compiler_params=pltpu.CompilerParams(
            collective_id=0, has_side_effects=True, vmem_limit_bytes=66000000),
    )(counts, chosen, gates, tokens, w_gate, w_up, w_down)
    return jnp.dot(place, answers, preferred_element_type=jnp.float32).astype(bf16)


def solution(mesh):
    in_specs = (
        P(("node", "local"), None),
        P("node", None, "local"),
        P("node", None, "local"),
        P("node", "local", None),
        P(),
        P(),
        P(),
    )
    out_specs = P(("node", "local"), None)
    body = functools.partial(shards, mesh.shape["node"], mesh.shape["local"])
    return jax.shard_map(body, mesh=mesh, in_specs=in_specs, out_specs=out_specs, check_vma=False)
```
